8 devices in a mesh: dp: 4 (over z, y, x), sp: 2 (over core).
Axes of the slice: x: 2, y: 2, z: 1, core: 2. Of those that a mesh axis runs over, the one named last changes fastest.
Arguments:
- act_in: bfloat16 [4, 4096, 1536], P('dp', 'sp')
- positions: int32 [4, 4096], P('dp', 'sp')
- out_grad: bfloat16 [4, 4096, 1536], P('dp', 'sp')
- norm1_gain: bfloat16 [1536], P(('dp', 'sp'))
- norm2_gain: bfloat16 [1536], P(('dp', 'sp'))
- w_query: bfloat16 [1536, 12, 128], P(('dp', 'sp'))
- w_key: bfloat16 [1536, 2, 128], P(('dp', 'sp'))
- w_value: bfloat16 [1536, 2, 128], P(('dp', 'sp'))
- w_out: bfloat16 [1536, 1536], P(('dp', 'sp'))
- w_gate: bfloat16 [1536, 8960], P(('dp', 'sp'))
- w_up: bfloat16 [1536, 8960], P(('dp', 'sp'))
- w_down: bfloat16 [8960, 1536], P(('dp', 'sp'))
Outputs:
- output 1: bfloat16 [4, 4096, 1536], P('dp', 'sp')
- output 2: bfloat16 [4, 4096, 1536], P('dp', 'sp')
- output 3: float32 [1536], P(('dp', 'sp'))
- output 4: float32 [1536], P(('dp', 'sp'))
- output 5: float32 [1536, 12, 128], P(('dp', 'sp'))
- output 6: float32 [1536, 2, 128], P(('dp', 'sp'))
- output 7: float32 [1536, 2, 128], P(('dp', 'sp'))
- output 8: float32 [1536, 1536], P(('dp', 'sp'))
- output 9: float32 [1536, 8960], P(('dp', 'sp'))
- output 10: float32 [1536, 8960], P(('dp', 'sp'))
- output 11: float32 [8960, 1536], P(('dp', 'sp'))
All inputs are finite; a program needn't handle non-finite values.
Results may differ from the reference program's by a relative error of at most 0.0153044.
Values are sent between devices in bfloat16 or wider.
A program may use at most 1 GiB of HBM per device.

```python
import math
import jax
import jax.numpy as jnp
from jax import lax

MODEL_DIM = 1536
Q_HEADS = 12
KV_HEADS = 2
HEAD_DIM = 128
FFN_DIM = 8960
TOKENS_DEV = 2048
DP_SIZE = 4
SP_SIZE = 2

SEQ_LEN = TOKENS_DEV * SP_SIZE
HALF_DIM = HEAD_DIM // 2
N_GROUP = Q_HEADS // KV_HEADS
Q_BLOCK = math.gcd(SEQ_LEN, 256)
N_BLOCKS = SEQ_LEN // Q_BLOCK
ATTN_SCALE = HEAD_DIM ** -0.5
EPS = 1e-5
ROPE_BASE = 10000.0
QK_GAIN = 1.5
NEG_BIG = -1e30


def draw_weight(draw_key, shape, fan_in, gain_factor):
    return (jax.random.normal(draw_key, shape, jnp.float32) * (gain_factor * fan_in ** -0.5)).astype(jnp.bfloat16)


def setup_inputs(seed: int = 0) -> dict:
    key_list = jax.random.split(jax.random.key(seed), 12)
    row_shape = (DP_SIZE, SEQ_LEN, MODEL_DIM)
    q_width = Q_HEADS * HEAD_DIM
    pos_steps = jax.random.randint(key_list[1], (DP_SIZE, SEQ_LEN), 1, 3)
    return dict(
        act_in=jax.random.normal(key_list[0], row_shape, jnp.float32).astype(jnp.bfloat16),
        positions=(jnp.cumsum(pos_steps, axis=1) - 1).astype(jnp.int32),
        out_grad=jax.random.normal(key_list[2], row_shape, jnp.float32).astype(jnp.bfloat16),
        norm1_gain=jax.random.uniform(key_list[3], (MODEL_DIM,), jnp.float32, 0.5, 1.5).astype(jnp.bfloat16),
        norm2_gain=jax.random.uniform(key_list[4], (MODEL_DIM,), jnp.float32, 0.5, 1.5).astype(jnp.bfloat16),
        w_query=draw_weight(key_list[5], (MODEL_DIM, Q_HEADS, HEAD_DIM), MODEL_DIM, QK_GAIN),
        w_key=draw_weight(key_list[6], (MODEL_DIM, KV_HEADS, HEAD_DIM), MODEL_DIM, QK_GAIN),
        w_value=draw_weight(key_list[7], (MODEL_DIM, KV_HEADS, HEAD_DIM), MODEL_DIM, 1.0),
        w_out=draw_weight(key_list[8], (q_width, MODEL_DIM), q_width, 1.0),
        w_gate=draw_weight(key_list[9], (MODEL_DIM, FFN_DIM), MODEL_DIM, 1.0),
        w_up=draw_weight(key_list[10], (MODEL_DIM, FFN_DIM), MODEL_DIM, 1.0),
        w_down=draw_weight(key_list[11], (FFN_DIM, MODEL_DIM), FFN_DIM, 1.0),
    )


def rms_scale(rows_f32):
    return lax.rsqrt(jnp.mean(rows_f32 * rows_f32, axis=-1, keepdims=True) + EPS)


def to_bf(values):
    return values.astype(jnp.bfloat16).astype(jnp.float32)


def rope_apply(values, positions):
    inv_freq = ROPE_BASE ** (-(jnp.arange(HALF_DIM, dtype=jnp.float32) * (2.0 / HEAD_DIM)))
    angles = positions.astype(jnp.float32)[:, None] * inv_freq[None, :]
    cos_t = jnp.cos(angles)[:, None, :]
    sin_t = jnp.sin(angles)[:, None, :]
    first_half = values[..., :HALF_DIM]
    second_half = values[..., HALF_DIM:]
    return jnp.concatenate([first_half * cos_t - second_half * sin_t, second_half * cos_t + first_half * sin_t], axis=-1)


def layer_forward(weights, act_rows, positions):
    gain_a, gain_b, w_query, w_key, w_value, w_out, w_gate, w_up, w_down = weights
    act_f = act_rows.astype(jnp.float32)
    normed_a = to_bf(act_f * rms_scale(act_f) * gain_a)
    q_rot = to_bf(rope_apply(jnp.einsum("sd,dhe->she", normed_a, w_query), positions))
    k_rot = to_bf(rope_apply(jnp.einsum("sd,dhe->she", normed_a, w_key), positions))
    v_proj = to_bf(jnp.einsum("sd,dhe->she", normed_a, w_value))
    q_groups = q_rot.reshape(N_BLOCKS, Q_BLOCK, KV_HEADS, N_GROUP, HEAD_DIM)
    block_starts = jnp.arange(N_BLOCKS) * Q_BLOCK
    key_index = jnp.arange(SEQ_LEN)

    def one_block(block_item):
        q_blk, q_start = block_item
        scores = jnp.einsum("qkgd,skd->kgqs", q_blk, k_rot) * ATTN_SCALE
        allowed = (q_start + jnp.arange(Q_BLOCK))[:, None] >= key_index[None, :]
        scores = jnp.where(allowed, scores, NEG_BIG)
        prob_rows = to_bf(jax.nn.softmax(scores, axis=-1))
        return to_bf(jnp.einsum("kgqs,skd->qkgd", prob_rows, v_proj))

    attn_rows = lax.map(jax.checkpoint(one_block), (q_groups, block_starts)).reshape(SEQ_LEN, Q_HEADS * HEAD_DIM)
    hidden = to_bf(act_f + jnp.dot(attn_rows, w_out))
    normed_b = to_bf(hidden * rms_scale(hidden) * gain_b)
    mixed_act = to_bf(jax.nn.silu(jnp.dot(normed_b, w_gate)) * jnp.dot(normed_b, w_up))
    return (hidden + jnp.dot(mixed_act, w_down)).astype(jnp.bfloat16)


def reference(act_in, positions, out_grad, norm1_gain, norm2_gain, w_query, w_key, w_value, w_out, w_gate, w_up, w_down):
    weights = tuple(param.astype(jnp.float32) for param in (norm1_gain, norm2_gain, w_query, w_key, w_value, w_out, w_gate, w_up, w_down))
    zero_grads = tuple(jnp.zeros_like(param) for param in weights)

    def per_sequence(grad_sums, seq_item):
        act_row, pos_row, grad_row = seq_item

        def fwd_fn(params, act_rows):
            return layer_forward(params, act_rows, pos_row)

        act_out, pullback = jax.vjp(fwd_fn, weights, act_row)
        param_grads, act_grad = pullback(grad_row)
        new_sums = tuple(run_sum + seq_grad for run_sum, seq_grad in zip(grad_sums, param_grads))
        return new_sums, (act_out, act_grad)

    grad_sums, outs = lax.scan(per_sequence, zero_grads, (act_in, positions, out_grad))
    return (outs[0], outs[1], grad_sums[0], grad_sums[1], grad_sums[2], grad_sums[3], grad_sums[4], grad_sums[5], grad_sums[6], grad_sums[7], grad_sums[8])
```

```python
import jax
import jax.numpy as jnp
from jax import lax
from jax.experimental import pallas as pl
from jax.experimental.pallas import tpu as pltpu
from jax.sharding import PartitionSpec as P


EPS = 1e-5
ROPE_BASE = 10000.0
NEG_BIG = -1e30
LOG2E = 1.4426950408889634
F32 = jnp.float32
BF16 = jnp.bfloat16

HD = 128
VMEM_LIMIT = 60 * 1024 * 1024
NT = (((1,), (1,)), ((), ()))


def dot(a, b):
    return jnp.dot(a, b, preferred_element_type=F32)


def dot_nt(a, b):
    return lax.dot_general(a, b, NT, preferred_element_type=F32)


def cost(flops, nbytes, trans=0):
    return pl.CostEstimate(flops=int(flops), bytes_accessed=int(nbytes), transcendentals=int(trans))


def qkv_kernel(x_ref, g_ref, w_ref, cos_ref, sin_ref, out_ref, u_ref):
    x = x_ref[...].astype(F32)
    scale = lax.rsqrt(jnp.mean(x * x, axis=-1, keepdims=True) + EPS)
    u = (x * scale * g_ref[...]).astype(BF16)
    u_ref[...] = u
    cos = cos_ref[...]
    sin = sin_ref[...]
    cols = w_ref.shape[1]
    step = 512
    per_core = cols // 2
    for n in range(cols // step):
        a = dot(u, w_ref[:, n * step:(n + 1) * step])
        for h in range(step // HD):
            col = n * step + h * HD
            part = a[:, h * HD:(h + 1) * HD]
            if (col % per_core) < per_core - HD:
                part = part * cos + pltpu.roll(part, HD // 2, 1) * sin
            out_ref[:, col:col + HD] = part.astype(BF16)


def qkv_project(x, gain, w_qkv, cos, sin):
    rows, dim = x.shape
    cols = w_qkv.shape[1]
    bm = 512
    return pl.pallas_call(
        qkv_kernel,
        grid=(rows // bm,),
        in_specs=[
            pl.BlockSpec((bm, dim), lambda i: (i, 0)),
            pl.BlockSpec((1, dim), lambda i: (0, 0)),
            pl.BlockSpec((dim, cols), lambda i: (0, 0)),
            pl.BlockSpec((bm, HD), lambda i: (i, 0)),
            pl.BlockSpec((bm, HD), lambda i: (i, 0)),
        ],
        out_specs=[pl.BlockSpec((bm, cols), lambda i: (i, 0)), pl.BlockSpec((bm, dim), lambda i: (i, 0))],
        out_shape=[jax.ShapeDtypeStruct((rows, cols), BF16), jax.ShapeDtypeStruct((rows, dim), BF16)],
        compiler_params=pltpu.CompilerParams(vmem_limit_bytes=VMEM_LIMIT),
        cost_estimate=cost(2 * rows * dim * cols, 2 * (2 * rows * dim + dim * cols + rows * cols)),
        name="qkv_project",
    )(x, gain, w_qkv, cos, sin)


BQ = 256
BK = 512


def attn_fwd_kernel(c_ref, q_ref, k_ref, v_ref, o_ref, lse_ref, vt_ref, m_ref, l_ref, acc_ref):
    i = pl.program_id(0)
    seq = k_ref.shape[0]
    n_kb = seq // BK
    n_head = q_ref.shape[1] // HD
    coef = HD ** -0.5 * LOG2E
    shift = c_ref[0] * (n_kb // 2)

    def phys(j):
        return pl.multiple_of(lax.rem(j + shift, n_kb) * BK, BK)

    @pl.when(i == 0)
    def _():
        for j in range(n_kb):
            vt_ref[j] = v_ref[pl.ds(phys(j), BK), :].astype(F32).T.astype(BF16)

    m_ref[...] = jnp.full_like(m_ref, NEG_BIG)
    l_ref[...] = jnp.zeros_like(l_ref)
    acc_ref[...] = jnp.zeros_like(acc_ref)

    def block(j, masked):
        k_blk = k_ref[pl.ds(phys(j), BK), :]
        vt = vt_ref[j]
        if masked:
            keys = j * BK + lax.broadcasted_iota(jnp.int32, (BK, BQ), 0)
            queries = i * BQ + lax.broadcasted_iota(jnp.int32, (BK, BQ), 1)
            allowed = keys <= queries
        for h in range(n_head):
            t = dot_nt(k_blk, q_ref[:, h * HD:(h + 1) * HD]) * coef
            if masked:
                t = jnp.where(allowed, t, NEG_BIG)
            m_prev = m_ref[h]
            m_new = jnp.maximum(m_prev, jnp.max(t, axis=0, keepdims=True))
            p = jnp.exp2(t - m_new)
            alpha = jnp.exp2(m_prev - m_new)
            m_ref[h] = m_new
            l_ref[h] = l_ref[h] * alpha + jnp.sum(p, axis=0, keepdims=True)
            acc_ref[h] = acc_ref[h] * alpha + dot(vt, p.astype(BF16))

    last = (i * BQ) // BK

    def body(j, carry):
        block(j, False)
        return carry

    lax.fori_loop(0, last, body, 0)
    block(last, True)
    for h in range(n_head):
        total = l_ref[h]
        o_ref[:, h * HD:(h + 1) * HD] = (acc_ref[h] / total).T.astype(BF16)
        lse_ref[0, h:h + 1, :] = m_ref[h] + jnp.log2(total)
    lse_ref[0, n_head:, :] = jnp.zeros_like(lse_ref[0, n_head:, :])


def attn_forward(core, qkv):
    seq, width = qkv.shape
    qw = width - 2 * HD
    n_head = qw // HD
    n_q = seq // BQ

    def rows(i, c):
        return (lax.rem(i + c[0] * (n_q // 2), n_q), 0)

    pairs = seq * seq // 2 * n_head
    return pl.pallas_call(
        attn_fwd_kernel,
        grid_spec=pltpu.PrefetchScalarGridSpec(
            num_scalar_prefetch=1,
            grid=(n_q,),
            in_specs=[
                pl.BlockSpec((BQ, qw), rows),
                pl.BlockSpec((seq, HD), lambda i, c: (0, n_head)),
                pl.BlockSpec((seq, HD), lambda i, c: (0, n_head + 1)),
            ],
            out_specs=[pl.BlockSpec((BQ, qw), rows), pl.BlockSpec((1, 8, BQ), lambda i, c: (i, 0, 0))],
            scratch_shapes=[
                pltpu.VMEM((seq // BK, HD, BK), BF16),
                pltpu.VMEM((n_head, 1, BQ), F32),
                pltpu.VMEM((n_head, 1, BQ), F32),
                pltpu.VMEM((n_head, HD, BQ), F32),
            ],
        ),
        out_shape=[jax.ShapeDtypeStruct((seq, qw), BF16), jax.ShapeDtypeStruct((n_q, 8, BQ), F32)],
        compiler_params=pltpu.CompilerParams(vmem_limit_bytes=VMEM_LIMIT),
        cost_estimate=cost(8 * pairs * HD, 4 * seq * width, pairs),
        name="attn_forward",
    )(core, qkv, qkv, qkv)


def attn_bwd_kernel(c_ref, q_ref, do_ref, o_ref, lse_ref, cos_ref, sin_ref, k_ref, v_ref, cos_all_ref, sin_all_ref,
                    dq_ref, dkv_ref, kt_ref, dqt_ref, delta_ref, dk_ref, dv_ref):
    i = pl.program_id(0)
    seq = k_ref.shape[0]
    n_kb = seq // BK
    n_head = q_ref.shape[1] // HD
    attn_scale = HD ** -0.5
    coef = attn_scale * LOG2E
    shift = c_ref[0] * (n_kb // 2)

    def phys(j):
        return pl.multiple_of(lax.rem(j + shift, n_kb) * BK, BK)

    @pl.when(i == 0)
    def _():
        for j in range(n_kb):
            kt_ref[j] = k_ref[pl.ds(phys(j), BK), :].astype(F32).T.astype(BF16)
        dk_ref[...] = jnp.zeros_like(dk_ref)
        dv_ref[...] = jnp.zeros_like(dv_ref)

    dqt_ref[...] = jnp.zeros_like(dqt_ref)
    for h in range(n_head):
        cols = slice(h * HD, (h + 1) * HD)
        prod = do_ref[:, cols].astype(F32) * o_ref[:, cols].astype(F32)
        delta_ref[h] = jnp.sum(prod.T, axis=0, keepdims=True)

    def block(j, masked):
        k_blk = k_ref[pl.ds(phys(j), BK), :]
        v_blk = v_ref[pl.ds(phys(j), BK), :]
        kt = kt_ref[j]
        dk = dk_ref[j]
        dv = dv_ref[j]
        if masked:
            keys = j * BK + lax.broadcasted_iota(jnp.int32, (BK, BQ), 0)
            queries = i * BQ + lax.broadcasted_iota(jnp.int32, (BK, BQ), 1)
            allowed = keys <= queries
        for h in range(n_head):
            cols = slice(h * HD, (h + 1) * HD)
            q_h = q_ref[:, cols]
            do_h = do_ref[:, cols]
            t = dot_nt(k_blk, q_h) * coef
            if masked:
                t = jnp.where(allowed, t, NEG_BIG)
            p = jnp.exp2(t - lse_ref[0, h:h + 1, :])
            ds = (p * (dot_nt(v_blk, do_h) - delta_ref[h])).astype(BF16)
            dv = dv + dot(p.astype(BF16), do_h)
            dk = dk + dot(ds, q_h)
            dqt_ref[h] = dqt_ref[h] + dot(kt, ds)
        dk_ref[j] = dk
        dv_ref[j] = dv

    last = (i * BQ) // BK

    def body(j, carry):
        block(j, False)
        return carry

    lax.fori_loop(0, last, body, 0)
    block(last, True)

    def unrotate(grad, cos, sin):
        grad = grad.astype(BF16).astype(F32)
        return (grad * cos - pltpu.roll(grad, HD // 2, 1) * sin).astype(BF16)

    for h in range(n_head):
        dq_ref[:, h * HD:(h + 1) * HD] = unrotate((dqt_ref[h] * attn_scale).T, cos_ref[...], sin_ref[...])

    @pl.when(i == pl.num_programs(0) - 1)
    def _():
        for j in range(n_kb):
            at = pl.ds(phys(j), BK)
            dkv_ref[at, :HD] = unrotate(dk_ref[j] * attn_scale, cos_all_ref[at, :], sin_all_ref[at, :])
            dkv_ref[at, HD:] = dv_ref[j].astype(BF16)


def attn_backward(core, qkv, grad_out, out, lse, cos, sin):
    seq, width = qkv.shape
    qw = width - 2 * HD
    n_head = qw // HD
    n_q = seq // BQ

    def rows(i, c):
        return (lax.rem(i + c[0] * (n_q // 2), n_q), 0)

    def whole(i, c):
        return (0, 0)

    pairs = seq * seq // 2 * n_head
    return pl.pallas_call(
        attn_bwd_kernel,
        grid_spec=pltpu.PrefetchScalarGridSpec(
            num_scalar_prefetch=1,
            grid=(n_q,),
            in_specs=[
                pl.BlockSpec((BQ, qw), rows),
                pl.BlockSpec((BQ, qw), rows),
                pl.BlockSpec((BQ, qw), rows),
                pl.BlockSpec((1, 8, BQ), lambda i, c: (i, 0, 0)),
                pl.BlockSpec((BQ, HD), rows),
                pl.BlockSpec((BQ, HD), rows),
                pl.BlockSpec((seq, HD), lambda i, c: (0, n_head)),
                pl.BlockSpec((seq, HD), lambda i, c: (0, n_head + 1)),
                pl.BlockSpec((seq, HD), whole),
                pl.BlockSpec((seq, HD), whole),
            ],
            out_specs=[pl.BlockSpec((BQ, qw), rows), pl.BlockSpec((seq, 2 * HD), whole)],
            scratch_shapes=[
                pltpu.VMEM((seq // BK, HD, BK), BF16),
                pltpu.VMEM((n_head, HD, BQ), F32),
                pltpu.VMEM((n_head, 1, BQ), F32),
                pltpu.VMEM((seq // BK, BK, HD), F32),
                pltpu.VMEM((seq // BK, BK, HD), F32),
            ],
        ),
        out_shape=[jax.ShapeDtypeStruct((seq, qw), BF16), jax.ShapeDtypeStruct((seq, 2 * HD), BF16)],
        compiler_params=pltpu.CompilerParams(vmem_limit_bytes=VMEM_LIMIT),
        cost_estimate=cost(20 * pairs * HD, 8 * seq * width, pairs),
        name="attn_backward",
    )(core, qkv, grad_out, out, lse, cos, sin, qkv, qkv, cos, sin)


FT = 640


def ffn_kernel(w_ref, dy_ref, w13_ref, w2_ref, mix_ref, dgu_ref):
    pre = dot(w_ref[...], w13_ref[...])
    dmix = dot_nt(dy_ref[...], w2_ref[...]).astype(BF16).astype(F32)
    gate = pre[:, :FT]
    up = pre[:, FT:]
    sig = jax.nn.sigmoid(gate)
    act = gate * sig
    mix_ref[...] = (act * up).astype(BF16)
    dgu_ref[:, :FT] = (dmix * up * sig * (1.0 + gate * (1.0 - sig))).astype(BF16)
    dgu_ref[:, FT:] = (dmix * act).astype(BF16)


def ffn_chunk(w, dy, w13, w2):
    rows, dim = w.shape
    cols = w2.shape[0]
    bm = 512
    return pl.pallas_call(
        ffn_kernel,
        grid=(cols // FT, rows // bm),
        in_specs=[
            pl.BlockSpec((bm, dim), lambda f, i: (i, 0)),
            pl.BlockSpec((bm, dim), lambda f, i: (i, 0)),
            pl.BlockSpec((dim, 2 * FT), lambda f, i: (0, f)),
            pl.BlockSpec((FT, dim), lambda f, i: (f, 0)),
        ],
        out_specs=[pl.BlockSpec((bm, FT), lambda f, i: (i, f)), pl.BlockSpec((bm, 2 * FT), lambda f, i: (i, f))],
        out_shape=[jax.ShapeDtypeStruct((rows, cols), BF16), jax.ShapeDtypeStruct((rows, 2 * cols), BF16)],
        compiler_params=pltpu.CompilerParams(vmem_limit_bytes=VMEM_LIMIT),
        cost_estimate=cost(6 * rows * dim * cols, 2 * (4 * rows * dim + 3 * dim * cols + 3 * rows * cols), rows * cols),
        name="ffn_chunk",
    )(w, dy, w13, w2)


def rms_backward(grad_normed, rows_f32, gain_f32):
    row_scale = lax.rsqrt(jnp.mean(rows_f32 * rows_f32, axis=-1, keepdims=True) + EPS)
    unit_rows = rows_f32 * row_scale
    gain_grad = jnp.sum(grad_normed * unit_rows, axis=0)
    grad_unit = grad_normed * gain_f32
    inner_mean = jnp.mean(grad_unit * unit_rows, axis=-1, keepdims=True)
    return row_scale * (grad_unit - unit_rows * inner_mean), gain_grad


def solution(mesh):
    flat_axes = ("dp", "sp")
    row_spec = P("dp", "sp", None)
    pos_spec = P("dp", "sp")
    vec_spec = P(flat_axes)
    mat_spec = P(flat_axes, None)
    cube_spec = P(flat_axes, None, None)
    n_dp = mesh.shape["dp"]

    def swap(values):
        return lax.ppermute(values, "sp", [(0, 1), (1, 0)])

    def gather_dp(values):
        return lax.all_gather(values, "dp", axis=0, tiled=True)

    def gather_all(values):
        return lax.all_gather(values, flat_axes, axis=0, tiled=True)

    def scatter_dp(values):
        return lax.psum_scatter(values, "dp", scatter_dimension=0, tiled=True)

    def scatter_all(values):
        return lax.psum_scatter(values, flat_axes, scatter_dimension=0, tiled=True)

    def layer(act_in, positions, out_grad, norm1_gain, norm2_gain, w_query, w_key, w_value, w_out, w_gate, w_up, w_down):
        core = lax.axis_index("sp")
        first = core == 0
        core_arr = jnp.full((1,), core, jnp.int32)
        rows = act_in.shape[1]
        shard = w_query.shape[0]
        n_head = w_query.shape[1]
        n_kv = w_key.shape[1]
        hpc = n_head // n_kv
        qw = hpc * HD
        fshard = w_down.shape[0]
        x = act_in[0]
        dy = out_grad[0]

        def in_order(mine, other, axis):
            return jnp.where(first, jnp.concatenate([mine, other], axis), jnp.concatenate([other, mine], axis))

        wq = w_query.reshape(shard, n_head * HD)
        parts = []
        for g in range(n_kv):
            parts += [wq[:, g * qw:(g + 1) * qw], w_key[:, g, :], w_value[:, g, :]]
        parts += [norm1_gain[:, None], norm2_gain[:, None], jnp.zeros((shard, HD - 2), BF16)]
        packed = gather_all(jnp.concatenate(parts, axis=1))
        n_qkv = n_kv * (qw + 2 * HD)
        w_qkv = packed[:, :n_qkv]
        gain1 = packed[:, n_qkv].astype(F32)
        gain2 = packed[:, n_qkv + 1].astype(F32)
        wo = gather_all(w_out)

        r_cuts = ((0, fshard * 3 // 7), (fshard * 3 // 7, fshard))

        def columns(mat, part, cut):
            return jnp.concatenate([mat[:, (2 * d + part) * fshard + cut[0]:(2 * d + part) * fshard + cut[1]] for d in range(n_dp)], axis=1)

        def pack13(part, cut):
            gate = columns(w_gate, part, cut)
            up = columns(w_up, part, cut)
            tiles = []
            for t in range(gate.shape[1] // FT):
                tiles += [gate[:, t * FT:(t + 1) * FT], up[:, t * FT:(t + 1) * FT]]
            return jnp.concatenate(tiles, axis=1)

        w13 = []
        w2 = []
        for cut in r_cuts:
            pack_a = pack13(0, cut)
            pack_b = pack13(1, cut)
            mine = jnp.where(first, pack_a, pack_b)
            other = jnp.where(first, pack_b, pack_a)
            w13.append(gather_dp(in_order(mine, swap(other), 0)))
            w2.append(gather_dp(w_down[cut[0]:cut[1]]))

        dy_full = jnp.concatenate([dy, swap(dy)], axis=0)
        pos_full = jnp.concatenate([positions[0], swap(positions[0])], axis=0)
        inv_freq = ROPE_BASE ** (-(jnp.arange(HD // 2, dtype=F32) * (2.0 / HD)))
        angles = pos_full.astype(F32)[:, None] * inv_freq[None, :]
        cos_h = jnp.cos(angles)
        sin_h = jnp.sin(angles)
        cos = jnp.concatenate([cos_h, cos_h], axis=1)
        sin = jnp.concatenate([-sin_h, sin_h], axis=1)

        qkv, normed_a = qkv_project(x, gain1[None, :], w_qkv, cos, sin)
        half = n_qkv // 2
        qkv_mine = jnp.where(first, qkv[:, :half], qkv[:, half:])
        qkv_other = jnp.where(first, qkv[:, half:], qkv[:, :half])
        qkv_seq = jnp.concatenate([qkv_mine, swap(qkv_other)], axis=0)
        attn_seq, lse = attn_forward(core_arr, qkv_seq)
        attn_flat = in_order(attn_seq[:rows], swap(attn_seq[rows:]), 1)
        x_f = x.astype(F32)
        hidden = (x_f + dot(attn_flat, wo)).astype(BF16)
        hidden_f = hidden.astype(F32)
        scale_b = lax.rsqrt(jnp.mean(hidden_f * hidden_f, axis=-1, keepdims=True) + EPS)
        normed_b = (hidden_f * scale_b * gain2).astype(BF16)
        normed_full = jnp.concatenate([normed_b, swap(normed_b)], axis=0)

        tn = (((0,), (0,)), ((), ()))
        mixed = []
        dgu = []
        down_parts = []
        gu_parts = []
        for k in range(len(r_cuts)):
            mix_k, dgu_k = ffn_chunk(normed_full, dy_full, w13[k], w2[k])
            mixed.append(mix_k)
            dgu.append(dgu_k)
            down_k = lax.dot_general(mix_k, dy_full, tn, preferred_element_type=F32)
            gu_k = lax.dot_general(normed_full, dgu_k, tn, preferred_element_type=F32)
            down_parts.append(scatter_dp(down_k))
            gu_parts.append(scatter_dp(gu_k))

        def grad_normed_part(lo, hi):
            return sum(dot_nt(dgu[k][lo:hi], w13[k]) for k in range(len(r_cuts)))

        grad_other = grad_normed_part(rows, 2 * rows)
        grad_other = swap(grad_other)
        grad_normed_b = (grad_normed_part(0, rows) + grad_other).astype(BF16).astype(F32)
        grad_rows_b, gain2_grad = rms_backward(grad_normed_b, hidden_f, gain2)
        grad_hidden = (dy.astype(F32) + grad_rows_b).astype(BF16)

        grad_attn = dot_nt(grad_hidden, wo).astype(BF16)
        ga_mine = jnp.where(first, grad_attn[:, :qw], grad_attn[:, qw:])
        ga_other = jnp.where(first, grad_attn[:, qw:], grad_attn[:, :qw])
        grad_attn_seq = jnp.concatenate([ga_mine, swap(ga_other)], axis=0)
        wout_part = lax.dot_general(attn_flat, grad_hidden, tn, preferred_element_type=F32)
        wout_grad = scatter_all(wout_part)
        dq, dkv = attn_backward(core_arr, qkv_seq, grad_attn_seq, attn_seq, lse, cos, sin)
        dqkv_mine = jnp.concatenate([dq[:rows], dkv[:rows]], axis=1)
        dqkv_other = swap(jnp.concatenate([dq[rows:], dkv[rows:]], axis=1))
        dqkv = in_order(dqkv_mine, dqkv_other, 1)
        qkv_part = lax.dot_general(normed_a, dqkv, tn, preferred_element_type=F32)
        qkv_grad = scatter_all(qkv_part)
        grad_normed_a = dot_nt(dqkv, w_qkv).astype(BF16).astype(F32)
        grad_rows_a, gain1_grad = rms_backward(grad_normed_a, x_f, gain1)
        in_grad = (grad_hidden.astype(F32) + grad_rows_a).astype(BF16)
        gain_grads = (scatter_all(gain1_grad), scatter_all(gain2_grad))

        def out_part(lo, hi):
            return sum(dot(mixed[k][lo:hi], w2[k]) for k in range(len(r_cuts)))

        out_other = out_part(rows, 2 * rows)
        act_out = (hidden_f + out_part(0, rows) + swap(out_other)).astype(BF16)

        down_grad = jnp.concatenate(down_parts, axis=0)
        gate_cols = []
        up_cols = []
        for k, cut in enumerate(r_cuts):
            top = gu_parts[k][:shard]
            bottom = gu_parts[k][shard:]
            mine = jnp.where(first, top, bottom)
            other = swap(jnp.where(first, bottom, top))
            by_core = (jnp.where(first, mine, other), jnp.where(first, other, mine))
            width = cut[1] - cut[0]
            gate_k = []
            up_k = []
            for arr in by_core:
                tiles = range(arr.shape[1] // (2 * FT))
                gate_k.append(jnp.concatenate([arr[:, 2 * t * FT:(2 * t + 1) * FT] for t in tiles], axis=1))
                up_k.append(jnp.concatenate([arr[:, (2 * t + 1) * FT:(2 * t + 2) * FT] for t in tiles], axis=1))
            gate_cols.append((gate_k, width))
            up_cols.append((up_k, width))

        def interleave(cols):
            pieces = []
            for d in range(n_dp):
                for part in range(2):
                    for arrs, width in cols:
                        pieces.append(arrs[part][:, d * width:(d + 1) * width])
            return jnp.concatenate(pieces, axis=1)

        gate_grad = interleave(gate_cols)
        up_grad = interleave(up_cols)
        per = qw + 2 * HD
        query_grad = jnp.concatenate([qkv_grad[:, g * per:g * per + qw] for g in range(n_kv)], axis=1).reshape(shard, n_head, HD)
        key_grad = jnp.stack([qkv_grad[:, g * per + qw:g * per + qw + HD] for g in range(n_kv)], axis=1)
        value_grad = jnp.stack([qkv_grad[:, g * per + qw + HD:(g + 1) * per] for g in range(n_kv)], axis=1)
        return (act_out[None], in_grad[None], gain_grads[0], gain_grads[1], query_grad, key_grad, value_grad, wout_grad, gate_grad, up_grad, down_grad)

    return jax.shard_map(layer, mesh=mesh, in_specs=(row_spec, pos_spec, row_spec, vec_spec, vec_spec, cube_spec, cube_spec, cube_spec, mat_spec, mat_spec, mat_spec, mat_spec), out_specs=(row_spec, row_spec, vec_spec, vec_spec, cube_spec, cube_spec, cube_spec, mat_spec, mat_spec, mat_spec, mat_spec), check_vma=False)
```

```python
import jax
import jax.numpy as jnp
from jax import lax
from jax.experimental import pallas as pl
from jax.experimental.pallas import tpu as pltpu
from jax.sharding import PartitionSpec as P


EPS = 1e-5
ROPE_BASE = 10000.0
NEG_BIG = -1e30
LOG2E = 1.4426950408889634
F32 = jnp.float32
BF16 = jnp.bfloat16

HD = 128
VMEM_LIMIT = 60 * 1024 * 1024
NT = (((1,), (1,)), ((), ()))


def dot(a, b):
    return jnp.dot(a, b, preferred_element_type=F32)


def dot_nt(a, b):
    return lax.dot_general(a, b, NT, preferred_element_type=F32)


def cost(flops, nbytes, trans=0):
    return pl.CostEstimate(flops=int(flops), bytes_accessed=int(nbytes), transcendentals=int(trans))


def qkv_kernel(x_ref, g_ref, w_ref, cos_ref, sin_ref, out_ref, u_ref):
    x = x_ref[...].astype(F32)
    scale = lax.rsqrt(jnp.mean(x * x, axis=-1, keepdims=True) + EPS)
    u = (x * scale * g_ref[...]).astype(BF16)
    u_ref[...] = u
    cos = cos_ref[...]
    sin = sin_ref[...]
    cols = w_ref.shape[1]
    step = 512
    per_core = cols // 2
    for n in range(cols // step):
        a = dot(u, w_ref[:, n * step:(n + 1) * step])
        for h in range(step // HD):
            col = n * step + h * HD
            part = a[:, h * HD:(h + 1) * HD]
            if (col % per_core) < per_core - HD:
                part = part * cos + pltpu.roll(part, HD // 2, 1) * sin
            out_ref[:, col:col + HD] = part.astype(BF16)


def qkv_project(x, gain, w_qkv, cos, sin):
    rows, dim = x.shape
    cols = w_qkv.shape[1]
    bm = 512
    return pl.pallas_call(
        qkv_kernel,
        grid=(rows // bm,),
        in_specs=[
            pl.BlockSpec((bm, dim), lambda i: (i, 0)),
            pl.BlockSpec((1, dim), lambda i: (0, 0)),
            pl.BlockSpec((dim, cols), lambda i: (0, 0)),
            pl.BlockSpec((bm, HD), lambda i: (i, 0)),
            pl.BlockSpec((bm, HD), lambda i: (i, 0)),
        ],
        out_specs=[pl.BlockSpec((bm, cols), lambda i: (i, 0)), pl.BlockSpec((bm, dim), lambda i: (i, 0))],
        out_shape=[jax.ShapeDtypeStruct((rows, cols), BF16), jax.ShapeDtypeStruct((rows, dim), BF16)],
        compiler_params=pltpu.CompilerParams(vmem_limit_bytes=VMEM_LIMIT),
        cost_estimate=cost(2 * rows * dim * cols, 2 * (2 * rows * dim + dim * cols + rows * cols)),
        name="qkv_project",
    )(x, gain, w_qkv, cos, sin)


BQ = 256
BQF = 512
BK = 512


def attn_fwd_kernel(c_ref, q_ref, k_ref, v_ref, o_ref, lse_ref, vt_ref, m_ref, l_ref, acc_ref):
    i = pl.program_id(0)
    seq = k_ref.shape[0]
    n_kb = seq // BK
    n_head = q_ref.shape[1] // HD
    coef = HD ** -0.5 * LOG2E
    shift = c_ref[0] * (n_kb // 2)

    def phys(j):
        return pl.multiple_of(lax.rem(j + shift, n_kb) * BK, BK)

    @pl.when(i == 0)
    def _():
        for j in range(n_kb):
            vt_ref[j] = v_ref[pl.ds(phys(j), BK), :].astype(F32).T.astype(BF16)

    m_ref[...] = jnp.full_like(m_ref, NEG_BIG)
    l_ref[...] = jnp.zeros_like(l_ref)
    acc_ref[...] = jnp.zeros_like(acc_ref)

    def block(j, masked):
        k_blk = k_ref[pl.ds(phys(j), BK), :]
        vt = vt_ref[j]
        if masked:
            keys = j * BK + lax.broadcasted_iota(jnp.int32, (BK, BQF), 0)
            queries = i * BQF + lax.broadcasted_iota(jnp.int32, (BK, BQF), 1)
            allowed = keys <= queries
        for h in range(n_head):
            t = dot_nt(k_blk, q_ref[:, h * HD:(h + 1) * HD]) * coef
            if masked:
                t = jnp.where(allowed, t, NEG_BIG)
            m_prev = m_ref[h]
            m_new = jnp.maximum(m_prev, jnp.max(t, axis=0, keepdims=True))
            p = jnp.exp2(t - m_new)
            alpha = jnp.exp2(m_prev - m_new)
            m_ref[h] = m_new
            l_ref[h] = l_ref[h] * alpha + jnp.sum(p, axis=0, keepdims=True)
            acc_ref[h] = acc_ref[h] * alpha + dot(vt, p.astype(BF16))

    last = (i * BQF) // BK

    def body(j, carry):
        block(j, False)
        return carry

    lax.fori_loop(0, last, body, 0)
    block(last, True)
    for h in range(n_head):
        total = l_ref[h]
        o_ref[:, h * HD:(h + 1) * HD] = (acc_ref[h] / total).T.astype(BF16)
        lse_ref[0, h:h + 1, :] = m_ref[h] + jnp.log2(total)
    lse_ref[0, n_head:, :] = jnp.zeros_like(lse_ref[0, n_head:, :])


def attn_forward(core, qkv):
    seq, width = qkv.shape
    qw = width - 2 * HD
    n_head = qw // HD
    n_q = seq // BQF

    def rows(i, c):
        return (lax.rem(i + c[0] * (n_q // 2), n_q), 0)

    pairs = seq * seq // 2 * n_head
    return pl.pallas_call(
        attn_fwd_kernel,
        grid_spec=pltpu.PrefetchScalarGridSpec(
            num_scalar_prefetch=1,
            grid=(n_q,),
            in_specs=[
                pl.BlockSpec((BQF, qw), rows),
                pl.BlockSpec((seq, HD), lambda i, c: (0, n_head)),
                pl.BlockSpec((seq, HD), lambda i, c: (0, n_head + 1)),
            ],
            out_specs=[pl.BlockSpec((BQF, qw), rows), pl.BlockSpec((1, 8, BQF), lambda i, c: (i, 0, 0))],
            scratch_shapes=[
                pltpu.VMEM((seq // BK, HD, BK), BF16),
                pltpu.VMEM((n_head, 1, BQF), F32),
                pltpu.VMEM((n_head, 1, BQF), F32),
                pltpu.VMEM((n_head, HD, BQF), F32),
            ],
        ),
        out_shape=[jax.ShapeDtypeStruct((seq, qw), BF16), jax.ShapeDtypeStruct((n_q, 8, BQF), F32)],
        compiler_params=pltpu.CompilerParams(vmem_limit_bytes=VMEM_LIMIT),
        cost_estimate=cost(8 * pairs * HD, 4 * seq * width, pairs),
        name="attn_forward",
    )(core, qkv, qkv, qkv)


def attn_bwd_kernel(c_ref, q_ref, do_ref, o_ref, lse_ref, cos_ref, sin_ref, k_ref, v_ref, cos_all_ref, sin_all_ref,
                    dq_ref, dkv_ref, kt_ref, dqt_ref, delta_ref, dk_ref, dv_ref):
    i = pl.program_id(0)
    seq = k_ref.shape[0]
    n_kb = seq // BK
    n_head = q_ref.shape[1] // HD
    attn_scale = HD ** -0.5
    coef = attn_scale * LOG2E
    shift = c_ref[0] * (n_kb // 2)

    def phys(j):
        return pl.multiple_of(lax.rem(j + shift, n_kb) * BK, BK)

    @pl.when(i == 0)
    def _():
        for j in range(n_kb):
            kt_ref[j] = k_ref[pl.ds(phys(j), BK), :].astype(F32).T.astype(BF16)
        dk_ref[...] = jnp.zeros_like(dk_ref)
        dv_ref[...] = jnp.zeros_like(dv_ref)

    dqt_ref[...] = jnp.zeros_like(dqt_ref)
    for h in range(n_head):
        cols = slice(h * HD, (h + 1) * HD)
        prod = do_ref[:, cols].astype(F32) * o_ref[:, cols].astype(F32)
        delta_ref[h] = jnp.sum(prod.T, axis=0, keepdims=True)

    def block(j, masked):
        k_blk = k_ref[pl.ds(phys(j), BK), :]
        v_blk = v_ref[pl.ds(phys(j), BK), :]
        kt = kt_ref[j]
        dk = dk_ref[j]
        dv = dv_ref[j]
        if masked:
            keys = j * BK + lax.broadcasted_iota(jnp.int32, (BK, BQ), 0)
            queries = i * BQ + lax.broadcasted_iota(jnp.int32, (BK, BQ), 1)
            allowed = keys <= queries
        for h in range(n_head):
            cols = slice(h * HD, (h + 1) * HD)
            q_h = q_ref[:, cols]
            do_h = do_ref[:, cols]
            t = dot_nt(k_blk, q_h) * coef
            if masked:
                t = jnp.where(allowed, t, NEG_BIG)
            p = jnp.exp2(t - lse_ref[0, h:h + 1, :])
            ds = (p * (dot_nt(v_blk, do_h) - delta_ref[h])).astype(BF16)
            dv = dv + dot(p.astype(BF16), do_h)
            dk = dk + dot(ds, q_h)
            dqt_ref[h] = dqt_ref[h] + dot(kt, ds)
        dk_ref[j] = dk
        dv_ref[j] = dv

    last = (i * BQ) // BK

    def body(j, carry):
        block(j, False)
        return carry

    lax.fori_loop(0, last, body, 0)
    block(last, True)

    def unrotate(grad, cos, sin):
        grad = grad.astype(BF16).astype(F32)
        return (grad * cos - pltpu.roll(grad, HD // 2, 1) * sin).astype(BF16)

    for h in range(n_head):
        dq_ref[:, h * HD:(h + 1) * HD] = unrotate((dqt_ref[h] * attn_scale).T, cos_ref[...], sin_ref[...])

    @pl.when(i == pl.num_programs(0) - 1)
    def _():
        for j in range(n_kb):
            at = pl.ds(phys(j), BK)
            dkv_ref[at, :HD] = unrotate(dk_ref[j] * attn_scale, cos_all_ref[at, :], sin_all_ref[at, :])
            dkv_ref[at, HD:] = dv_ref[j].astype(BF16)


def attn_backward(core, qkv, grad_out, out, lse, cos, sin):
    seq, width = qkv.shape
    qw = width - 2 * HD
    n_head = qw // HD
    n_q = seq // BQ

    def rows(i, c):
        return (lax.rem(i + c[0] * (n_q // 2), n_q), 0)

    def whole(i, c):
        return (0, 0)

    pairs = seq * seq // 2 * n_head
    return pl.pallas_call(
        attn_bwd_kernel,
        grid_spec=pltpu.PrefetchScalarGridSpec(
            num_scalar_prefetch=1,
            grid=(n_q,),
            in_specs=[
                pl.BlockSpec((BQ, qw), rows),
                pl.BlockSpec((BQ, qw), rows),
                pl.BlockSpec((BQ, qw), rows),
                pl.BlockSpec((1, 8, BQ), lambda i, c: (i // (BQF // BQ), 0, lax.rem(i, BQF // BQ))),
                pl.BlockSpec((BQ, HD), rows),
                pl.BlockSpec((BQ, HD), rows),
                pl.BlockSpec((seq, HD), lambda i, c: (0, n_head)),
                pl.BlockSpec((seq, HD), lambda i, c: (0, n_head + 1)),
                pl.BlockSpec((seq, HD), whole),
                pl.BlockSpec((seq, HD), whole),
            ],
            out_specs=[pl.BlockSpec((BQ, qw), rows), pl.BlockSpec((seq, 2 * HD), whole)],
            scratch_shapes=[
                pltpu.VMEM((seq // BK, HD, BK), BF16),
                pltpu.VMEM((n_head, HD, BQ), F32),
                pltpu.VMEM((n_head, 1, BQ), F32),
                pltpu.VMEM((seq // BK, BK, HD), F32),
                pltpu.VMEM((seq // BK, BK, HD), F32),
            ],
        ),
        out_shape=[jax.ShapeDtypeStruct((seq, qw), BF16), jax.ShapeDtypeStruct((seq, 2 * HD), BF16)],
        compiler_params=pltpu.CompilerParams(vmem_limit_bytes=VMEM_LIMIT),
        cost_estimate=cost(20 * pairs * HD, 8 * seq * width, pairs),
        name="attn_backward",
    )(core, qkv, grad_out, out, lse, cos, sin, qkv, qkv, cos, sin)


FT = 640


def ffn_kernel(w_ref, dy_ref, w13_ref, w2_ref, mix_ref, dgu_ref):
    pre = dot(w_ref[...], w13_ref[...])
    dmix = dot_nt(dy_ref[...], w2_ref[...]).astype(BF16).astype(F32)
    gate = pre[:, :FT]
    up = pre[:, FT:]
    sig = jax.nn.sigmoid(gate)
    act = gate * sig
    mix_ref[...] = (act * up).astype(BF16)
    dgu_ref[:, :FT] = (dmix * up * sig * (1.0 + gate * (1.0 - sig))).astype(BF16)
    dgu_ref[:, FT:] = (dmix * act).astype(BF16)


def ffn_chunk(w, dy, w13, w2):
    rows, dim = w.shape
    cols = w2.shape[0]
    bm = 512
    return pl.pallas_call(
        ffn_kernel,
        grid=(cols // FT, rows // bm),
        in_specs=[
            pl.BlockSpec((bm, dim), lambda f, i: (i, 0)),
            pl.BlockSpec((bm, dim), lambda f, i: (i, 0)),
            pl.BlockSpec((dim, 2 * FT), lambda f, i: (0, f)),
            pl.BlockSpec((FT, dim), lambda f, i: (f, 0)),
        ],
        out_specs=[pl.BlockSpec((bm, FT), lambda f, i: (i, f)), pl.BlockSpec((bm, 2 * FT), lambda f, i: (i, f))],
        out_shape=[jax.ShapeDtypeStruct((rows, cols), BF16), jax.ShapeDtypeStruct((rows, 2 * cols), BF16)],
        compiler_params=pltpu.CompilerParams(vmem_limit_bytes=VMEM_LIMIT),
        cost_estimate=cost(6 * rows * dim * cols, 2 * (4 * rows * dim + 3 * dim * cols + 3 * rows * cols), rows * cols),
        name="ffn_chunk",
    )(w, dy, w13, w2)


def rms_backward(grad_normed, rows_f32, gain_f32):
    row_scale = lax.rsqrt(jnp.mean(rows_f32 * rows_f32, axis=-1, keepdims=True) + EPS)
    unit_rows = rows_f32 * row_scale
    gain_grad = jnp.sum(grad_normed * unit_rows, axis=0)
    grad_unit = grad_normed * gain_f32
    inner_mean = jnp.mean(grad_unit * unit_rows, axis=-1, keepdims=True)
    return row_scale * (grad_unit - unit_rows * inner_mean), gain_grad


def solution(mesh):
    flat_axes = ("dp", "sp")
    row_spec = P("dp", "sp", None)
    pos_spec = P("dp", "sp")
    vec_spec = P(flat_axes)
    mat_spec = P(flat_axes, None)
    cube_spec = P(flat_axes, None, None)
    n_dp = mesh.shape["dp"]
    n_all = n_dp * mesh.shape["sp"]

    def swap(values):
        return lax.ppermute(values, "sp", [(0, 1), (1, 0)])

    def gather_dp(values):
        return lax.all_gather(values, "dp", axis=0, tiled=True)

    def gather_all(values):
        return lax.all_gather(values, flat_axes, axis=0, tiled=True)

    def scatter_dp(values):
        return lax.psum_scatter(values, "dp", scatter_dimension=0, tiled=True)

    def scatter_all(values):
        return lax.psum_scatter(values, flat_axes, scatter_dimension=0, tiled=True)

    def layer(act_in, positions, out_grad, norm1_gain, norm2_gain, w_query, w_key, w_value, w_out, w_gate, w_up, w_down):
        core = lax.axis_index("sp")
        first = core == 0
        core_arr = jnp.full((1,), core, jnp.int32)
        rows = act_in.shape[1]
        shard = w_query.shape[0]
        n_head = w_query.shape[1]
        n_kv = w_key.shape[1]
        hpc = n_head // n_kv
        qw = hpc * HD
        fshard = w_down.shape[0]
        x = act_in[0]
        dy = out_grad[0]

        def in_order(mine, other, axis):
            return jnp.where(first, jnp.concatenate([mine, other], axis), jnp.concatenate([other, mine], axis))

        wq = w_query.reshape(shard, n_head * HD)
        parts = []
        for g in range(n_kv):
            parts += [wq[:, g * qw:(g + 1) * qw], w_key[:, g, :], w_value[:, g, :]]
        parts += [norm1_gain[:, None], norm2_gain[:, None], jnp.zeros((shard, HD - 2), BF16)]
        packed = gather_all(jnp.concatenate(parts, axis=1))
        n_qkv = n_kv * (qw + 2 * HD)
        w_qkv = packed[:, :n_qkv]
        gain1 = packed[:, n_qkv].astype(F32)
        gain2 = packed[:, n_qkv + 1].astype(F32)
        wo = gather_all(w_out)

        r_cuts = ((0, fshard * 3 // 7), (fshard * 3 // 7, fshard))

        def columns(mat, part, cut):
            return jnp.concatenate([mat[:, (2 * d + part) * fshard + cut[0]:(2 * d + part) * fshard + cut[1]] for d in range(n_dp)], axis=1)

        def pack13(part, cut):
            gate = columns(w_gate, part, cut)
            up = columns(w_up, part, cut)
            tiles = []
            for t in range(gate.shape[1] // FT):
                tiles += [gate[:, t * FT:(t + 1) * FT], up[:, t * FT:(t + 1) * FT]]
            return jnp.concatenate(tiles, axis=1)

        w13 = []
        w2 = []
        for cut in r_cuts:
            pack_a = pack13(0, cut)
            pack_b = pack13(1, cut)
            mine = jnp.where(first, pack_a, pack_b)
            other = jnp.where(first, pack_b, pack_a)
            w13.append(gather_dp(in_order(mine, swap(other), 0)))
            w2.append(gather_dp(w_down[cut[0]:cut[1]]))

        dy_full = jnp.concatenate([dy, swap(dy)], axis=0)
        pos_full = jnp.concatenate([positions[0], swap(positions[0])], axis=0)
        inv_freq = ROPE_BASE ** (-(jnp.arange(HD // 2, dtype=F32) * (2.0 / HD)))
        angles = pos_full.astype(F32)[:, None] * inv_freq[None, :]
        cos_h = jnp.cos(angles)
        sin_h = jnp.sin(angles)
        cos = jnp.concatenate([cos_h, cos_h], axis=1)
        sin = jnp.concatenate([-sin_h, sin_h], axis=1)

        qkv, normed_a = qkv_project(x, gain1[None, :], w_qkv, cos, sin)
        half = n_qkv // 2
        qkv_mine = jnp.where(first, qkv[:, :half], qkv[:, half:])
        qkv_other = jnp.where(first, qkv[:, half:], qkv[:, :half])
        qkv_seq = jnp.concatenate([qkv_mine, swap(qkv_other)], axis=0)
        attn_seq, lse = attn_forward(core_arr, qkv_seq)
        attn_flat = in_order(attn_seq[:rows], swap(attn_seq[rows:]), 1)
        x_f = x.astype(F32)
        hidden = (x_f + dot(attn_flat, wo)).astype(BF16)
        hidden_f = hidden.astype(F32)
        scale_b = lax.rsqrt(jnp.mean(hidden_f * hidden_f, axis=-1, keepdims=True) + EPS)
        normed_b = (hidden_f * scale_b * gain2).astype(BF16)
        normed_full = jnp.concatenate([normed_b, swap(normed_b)], axis=0)

        tn = (((0,), (0,)), ((), ()))
        mixed = []
        dgu = []
        down_parts = []
        gu_parts = []
        for k in range(len(r_cuts)):
            mix_k, dgu_k = ffn_chunk(normed_full, dy_full, w13[k], w2[k])
            mixed.append(mix_k)
            dgu.append(dgu_k)
            down_k = lax.dot_general(mix_k, dy_full, tn, preferred_element_type=F32)
            gu_k = lax.dot_general(normed_full, dgu_k, tn, preferred_element_type=F32)
            down_parts.append(scatter_dp(down_k))
            gu_parts.append(scatter_dp(gu_k))

        def grad_normed_part(lo, hi):
            return sum(dot_nt(dgu[k][lo:hi], w13[k]) for k in range(len(r_cuts)))

        grad_other = grad_normed_part(rows, 2 * rows)
        grad_other = swap(grad_other)
        grad_normed_b = (grad_normed_part(0, rows) + grad_other).astype(BF16).astype(F32)
        grad_rows_b, gain2_grad = rms_backward(grad_normed_b, hidden_f, gain2)
        grad_hidden = (dy.astype(F32) + grad_rows_b).astype(BF16)

        grad_attn = dot_nt(grad_hidden, wo).astype(BF16)
        ga_mine = jnp.where(first, grad_attn[:, :qw], grad_attn[:, qw:])
        ga_other = jnp.where(first, grad_attn[:, qw:], grad_attn[:, :qw])
        grad_attn_seq = jnp.concatenate([ga_mine, swap(ga_other)], axis=0)
        wout_part = lax.dot_general(attn_flat, grad_hidden, tn, preferred_element_type=F32)
        wout_grad = scatter_all(wout_part)
        dq, dkv = attn_backward(core_arr, qkv_seq, grad_attn_seq, attn_seq, lse, cos, sin)
        normed_a_full = jnp.concatenate([normed_a, swap(normed_a)], axis=0)
        dqkv_seq = jnp.concatenate([dq, dkv], axis=1)
        qkv_part = lax.dot_general(normed_a_full, dqkv_seq, tn, preferred_element_type=F32)
        dqkv = in_order(dqkv_seq[:rows], swap(dqkv_seq[rows:]), 1)
        qkv_rows = scatter_dp(qkv_part)
        qkv_mine_rows = jnp.where(first, qkv_rows[:shard], qkv_rows[shard:])
        qkv_grad = in_order(qkv_mine_rows, swap(jnp.where(first, qkv_rows[shard:], qkv_rows[:shard])), 1)
        grad_normed_a = dot_nt(dqkv, w_qkv).astype(BF16).astype(F32)
        grad_rows_a, gain1_grad = rms_backward(grad_normed_a, x_f, gain1)
        in_grad = (grad_hidden.astype(F32) + grad_rows_a).astype(BF16)
        gain_sums = jnp.stack([gain1_grad, gain2_grad], axis=0)
        gain_sums = gain_sums + swap(gain_sums)
        bit = 1
        while bit < n_dp:
            gain_sums = gain_sums + lax.ppermute(gain_sums, "dp", [(d, d ^ bit) for d in range(n_dp)])
            bit *= 2
        me = lax.axis_index("dp") * (n_all // n_dp) + core
        gain_grads = lax.dynamic_slice_in_dim(gain_sums, me * shard, shard, axis=1)

        def out_part(lo, hi):
            return sum(dot(mixed[k][lo:hi], w2[k]) for k in range(len(r_cuts)))

        out_other = out_part(rows, 2 * rows)
        act_out = (hidden_f + out_part(0, rows) + swap(out_other)).astype(BF16)

        down_grad = jnp.concatenate(down_parts, axis=0)
        gate_cols = []
        up_cols = []
        for k, cut in enumerate(r_cuts):
            top = gu_parts[k][:shard]
            bottom = gu_parts[k][shard:]
            mine = jnp.where(first, top, bottom)
            other = swap(jnp.where(first, bottom, top))
            by_core = (jnp.where(first, mine, other), jnp.where(first, other, mine))
            width = cut[1] - cut[0]
            gate_k = []
            up_k = []
            for arr in by_core:
                tiles = range(arr.shape[1] // (2 * FT))
                gate_k.append(jnp.concatenate([arr[:, 2 * t * FT:(2 * t + 1) * FT] for t in tiles], axis=1))
                up_k.append(jnp.concatenate([arr[:, (2 * t + 1) * FT:(2 * t + 2) * FT] for t in tiles], axis=1))
            gate_cols.append((gate_k, width))
            up_cols.append((up_k, width))

        def interleave(cols):
            pieces = []
            for d in range(n_dp):
                for part in range(2):
                    for arrs, width in cols:
                        pieces.append(arrs[part][:, d * width:(d + 1) * width])
            return jnp.concatenate(pieces, axis=1)

        gate_grad = interleave(gate_cols)
        up_grad = interleave(up_cols)
        per = qw + 2 * HD
        query_grad = jnp.concatenate([qkv_grad[:, g * per:g * per + qw] for g in range(n_kv)], axis=1).reshape(shard, n_head, HD)
        key_grad = jnp.stack([qkv_grad[:, g * per + qw:g * per + qw + HD] for g in range(n_kv)], axis=1)
        value_grad = jnp.stack([qkv_grad[:, g * per + qw + HD:(g + 1) * per] for g in range(n_kv)], axis=1)
        return (act_out[None], in_grad[None], gain_grads[0], gain_grads[1], query_grad, key_grad, value_grad, wout_grad, gate_grad, up_grad, down_grad)

    return jax.shard_map(layer, mesh=mesh, in_specs=(row_spec, pos_spec, row_spec, vec_spec, vec_spec, cube_spec, cube_spec, cube_spec, mat_spec, mat_spec, mat_spec, mat_spec), out_specs=(row_spec, row_spec, vec_spec, vec_spec, cube_spec, cube_spec, cube_spec, mat_spec, mat_spec, mat_spec, mat_spec), check_vma=False)
```
